32 devices in a mesh: row: 8 (over z, y), col: 4 (over x, core).
Axes of the slice: x: 2, y: 2, z: 4, core: 2. Of those that a mesh axis runs over, the one named last changes fastest.
Arguments:
- new_dosage: float32 [4096, 1024], P(('col', 'row')), may hold values from 0 to 2
- old_dosage: float32 [16384, 1024], P(('row', 'col')), may hold values from 0 to 2
- grm: bfloat16 [16384, 4096], P('row', 'col'), may hold values from -1.5 to 1.5
- counts: int32 [8], P('col'), may hold values from 256 to 512
- affected: int32 [32, 8], P('row', 'col'), may hold values from 0 to 1, as said below
Outputs:
- updated: bfloat16 [16384, 4096], P('row', 'col')
The draws below stay inside these ranges and needn't reach their ends.
Inputs may be any that keep to these rules, and one draw needn't show every extreme that they name: `affected`: the density of marked tile pairs differs from one tile of new samples to the next.
All inputs are finite; a program needn't handle non-finite values.
Results may differ from the reference program's by a relative error of at most 0.00115.
Values may be sent and summed in bfloat16 or wider, within the bound.
No kernel may reach another device: no remote copies, remote signals or barrier semaphores. Data moves between devices by JAX's collectives and lax.ppermute only.
A program may use at most 128 MiB of HBM per device.

```python
import jax
import jax.numpy as jnp
from jax import lax

SNP = 1024
TILE = 512
REF_DEV = 2048
ALL = 16384
NEW = 4096
N_ROW = 8


def frequency_table(key):
    base_key, shift_key = jax.random.split(jax.random.fold_in(key, 5))
    base_rate = jax.random.uniform(base_key, (1, SNP), jnp.float32, 0.2, 0.8)
    shift_table = jax.random.uniform(shift_key, (16, SNP), jnp.float32, -0.15, 0.15)
    return base_rate + shift_table


def dosage_common(key, own_key, sample_count):
    frequency = frequency_table(key)
    subkeys = jax.random.split(own_key, 4)
    population = jax.random.randint(subkeys[0], (sample_count,), 0, 16)
    jitter = jax.random.uniform(subkeys[1], (sample_count, 1), jnp.float32, -0.02, 0.02)
    chance = jnp.clip(frequency[population] + jitter, 0.03, 0.97)
    allele_draw = jax.random.uniform(subkeys[2], (sample_count, SNP), jnp.float32, 0.0, 1.0)
    absent = (1.0 - chance) * (1.0 - chance)
    called = (allele_draw > absent).astype(jnp.float32) + (allele_draw > 1.0 - chance * chance).astype(jnp.float32)
    weight_draw = jax.random.uniform(subkeys[3], (sample_count, SNP), jnp.float32, 0.0, 1.0)
    shrinkage = 0.3 * weight_draw
    dosage = (1.0 - shrinkage) * called + shrinkage * 2.0 * chance
    return jnp.clip(dosage, 0.0, 2.0).astype(jnp.float32)


def draw_new_dosage(key, part):
    return dosage_common(key, jax.random.fold_in(key, 11), NEW)


def draw_old_dosage(key, part):
    return dosage_common(key, jax.random.fold_in(key, 23), ALL)


def draw_affected(key, part):
    first_key, second_key = jax.random.split(jax.random.fold_in(key, 37))
    offset = jax.random.randint(first_key, (), 0, 4)
    density = 1 + (jnp.arange(NEW // TILE) + offset) % 4
    tickets = jax.random.randint(second_key, (ALL // TILE, NEW // TILE), 0, 4)
    return (tickets < density[None, :]).astype(jnp.int32)


def touch_ends(drawn, key, least, top_value):
    dims = drawn.shape
    place = [jax.random.randint(jax.random.fold_in(key, axis), (), 0, dims[axis]) for axis in range(len(dims))]
    drawn = drawn.at[tuple(place)].set(least)
    longest = dims.index(max(dims))
    place[longest] = (place[longest] + 1) % dims[longest]
    return drawn.at[tuple(place)].set(top_value)


def level_of(key, shape, pieces, low, high):
    factor_of = 1.0
    for position, shards_of in pieces:
        draws = jax.random.uniform(jax.random.fold_in(jax.random.fold_in(key, 6), position), (shards_of,), jnp.float32, low / len(pieces), high / len(pieces))
        factor_of = factor_of * jnp.repeat(jnp.exp(draws), shape[position] // shards_of).reshape((-1,) + (1,) * (len(shape) - 1 - position))
    return factor_of


def gaussian(rng, shape, width, bound, cuts=(), held_as=jnp.bfloat16):
    values = width * jax.random.normal(rng, shape, jnp.float32)
    if cuts:
        values = values * level_of(rng, shape, cuts, -0.22, 0.18)
    return jnp.clip(values, -bound, bound).astype(held_as)


def setup_inputs(seed: int = 0) -> dict:
    arg_keys = jax.random.split(jax.random.key(seed), 6)
    new_dosage = draw_new_dosage(jax.random.fold_in(arg_keys[5], 71), 0)
    old_dosage = draw_old_dosage(jax.random.fold_in(arg_keys[5], 71), 0)
    grm = gaussian(arg_keys[2], (ALL, NEW), 0.1, 1.5, ((0, 8), (1, 4)))
    counts = touch_ends(jax.random.randint(arg_keys[3], (NEW // TILE,), TILE // 2, TILE + 1), jax.random.fold_in(arg_keys[3], 1), TILE // 2, TILE).astype(jnp.int32)
    affected = draw_affected(jax.random.fold_in(arg_keys[5], 71), 0)
    return {"new_dosage": new_dosage, "old_dosage": old_dosage, "grm": grm, "counts": counts, "affected": affected}


def reference(new_dosage, old_dosage, grm, counts, affected):
    totals = lax.optimization_barrier(jnp.sum(old_dosage, axis=0))
    doubled = totals / ALL
    spread = jnp.sqrt(doubled * (1.0 - 0.5 * doubled) + 0.1)
    usable = (jnp.arange(TILE)[None, :] < counts[:, None]).reshape(NEW).astype(jnp.float32)
    new_scores = ((new_dosage - doubled) / spread * usable[:, None]).astype(jnp.bfloat16)
    old_scores = ((old_dosage - doubled) / spread).astype(jnp.bfloat16)
    new_wide = new_scores.astype(jnp.float32)
    old_blocks = old_scores.reshape(N_ROW, REF_DEV, SNP)
    grm_blocks = grm.reshape(N_ROW, REF_DEV, NEW)
    mark_blocks = affected.reshape(N_ROW, REF_DEV // TILE, NEW // TILE)

    def update_block(operands):
        scores, grm_block, markers = operands
        product = jnp.dot(scores.astype(jnp.float32), new_wide.T, precision=lax.Precision.HIGHEST) / SNP
        spread_marks = jnp.repeat(jnp.repeat(markers.astype(jnp.float32), TILE, axis=0), TILE, axis=1)
        return (grm_block.astype(jnp.float32) + product * spread_marks).astype(jnp.bfloat16)
    updated = lax.map(update_block, (old_blocks, grm_blocks, mark_blocks))
    return updated.reshape(ALL, NEW)
```

```python
import functools

import jax
import jax.numpy as jnp
from jax import lax
from jax.experimental import pallas as pl
from jax.experimental.pallas import tpu as pltpu
from jax.sharding import PartitionSpec as P

TILE = 512
SCALE = 32767.0


def swap(value, axis, bits):
    size = lax.axis_size(axis)
    return lax.ppermute(value, axis, [(i, i ^ bits) for i in range(size)])


def to_fixed(x):
    return jnp.round((x - 1.0) * SCALE).astype(jnp.int32).astype(jnp.int16)


def pack_kernel(pieces, new_ref, old_ref, *out_refs):
    qnew_ref, *qold_refs, total_ref = out_refs
    qnew_ref[...] = to_fixed(new_ref[...])
    rows = old_ref.shape[0] // pieces
    total = jnp.zeros((1, old_ref.shape[1]), jnp.float32)
    for i, q_ref in enumerate(qold_refs):
        x = old_ref[i * rows:(i + 1) * rows, :]
        q_ref[...] = to_fixed(x)
        total = total + jnp.sum(x, axis=0, keepdims=True)
    total_ref[...] = total


def update_kernel(slots, pieces, chunk, all_count, place_ref, counts_ref, affected_ref, total_ref, *refs):
    n_new = len(slots[0])
    n_old = len(slots[1]) * pieces
    new_refs = refs[:n_new]
    old_refs = refs[n_new:n_new + n_old]
    grm_hbm, out_hbm, grm_ref, out_ref, score_ref, grm_sem, out_sem = refs[n_new + n_old:]
    snps = total_ref.shape[1]
    piece_rows = old_refs[0].shape[0]
    new_rows = new_refs[0].shape[0]
    row_me = place_ref[0]
    col_me = place_ref[1]

    def old_start(slot, piece):
        return ((col_me ^ slot) * pieces + piece) * piece_rows

    order = [(s, p) for s in slots[1] for p in range(pieces)]
    for i, (s, p) in enumerate(order):
        rows = pl.ds(pl.multiple_of(old_start(s, p), piece_rows), piece_rows)
        pltpu.make_async_copy(grm_hbm.at[rows], grm_ref.at[rows], grm_sem.at[i]).start()

    doubled = total_ref[...] / all_count
    inverse = lax.rsqrt(doubled * (1.0 - 0.5 * doubled) + 0.1)
    gain = inverse * (1.0 / SCALE)
    shift = (1.0 - doubled) * inverse

    for k, ref in zip(slots[0], new_refs):
        start = (row_me ^ k) * new_rows
        left = counts_ref[start // TILE] - start % TILE
        live = lax.broadcasted_iota(jnp.int32, (new_rows, 1), 0) < left
        score = ref[...].astype(jnp.int32).astype(jnp.float32) * gain + shift
        score = jnp.where(live, score, 0.0)
        score_ref[pl.ds(pl.multiple_of(start, new_rows), new_rows), :] = score.astype(jnp.bfloat16)

    cols = score_ref.shape[0]
    for i, (s, p) in enumerate(order):
        base = old_start(s, p)
        rows = pl.ds(pl.multiple_of(base, piece_rows), piece_rows)
        pltpu.make_async_copy(grm_hbm.at[rows], grm_ref.at[rows], grm_sem.at[i]).wait()
        old_ref = old_refs[i]

        def step(c, _):
            at = pl.multiple_of(c * chunk, chunk)
            to = pl.ds(pl.multiple_of(base + at, chunk), chunk)
            tile_row = (base + at) // TILE
            score = old_ref[pl.ds(at, chunk), :].astype(jnp.int32).astype(jnp.float32) * gain + shift
            score = score.astype(jnp.bfloat16)
            for t in range(cols // TILE):
                lanes = slice(t * TILE, (t + 1) * TILE)
                product = lax.dot_general(
                    score, score_ref[lanes, :], (((1,), (1,)), ((), ())), preferred_element_type=jnp.float32
                )
                weight = affected_ref[tile_row, t].astype(jnp.float32) * (1.0 / snps)
                out_ref[to, lanes] = (grm_ref[to, lanes].astype(jnp.float32) + product * weight).astype(jnp.bfloat16)
            return 0

        lax.fori_loop(0, piece_rows // chunk, step, 0)
        pltpu.make_async_copy(out_ref.at[rows], out_hbm.at[rows], out_sem.at[i]).start()
    for i, (s, p) in enumerate(order):
        rows = pl.ds(pl.multiple_of(old_start(s, p), piece_rows), piece_rows)
        pltpu.make_async_copy(out_ref.at[rows], out_hbm.at[rows], out_sem.at[i]).wait()


def on_device(new_dosage, old_dosage, grm, counts, affected):
    n_row, n_col = lax.axis_size("row"), lax.axis_size("col")
    old_rows, snps = old_dosage.shape
    new_rows = new_dosage.shape[0]
    pieces = 2
    piece_rows = old_rows // pieces
    vmem = pl.BlockSpec(memory_space=pltpu.VMEM)
    smem = pl.BlockSpec(memory_space=pltpu.SMEM)
    hbm = pl.BlockSpec(memory_space=pl.ANY)
    fixed = functools.partial(jax.ShapeDtypeStruct, dtype=jnp.int16)

    qnew, *rest = pl.pallas_call(
        functools.partial(pack_kernel, pieces),
        in_specs=[vmem, vmem],
        out_specs=[vmem] * (pieces + 2),
        out_shape=[fixed((new_rows, snps))]
        + [fixed((piece_rows, snps))] * pieces
        + [jax.ShapeDtypeStruct((1, snps), jnp.float32)],
        name="pack",
    )(new_dosage, old_dosage)
    qold, total = rest[:-1], rest[-1]

    old = {0: list(qold)}
    for k in range(2, n_col, 2):
        old[k] = [swap(q, "col", k) for q in qold]
    inner = 2 ** ((n_row.bit_length() - 1) // 2)
    new = {0: qnew}
    for k in range(inner, n_row, inner):
        new[k] = swap(qnew, "row", k)
    for axis, size in (("col", n_col), ("row", n_row)):
        bit = 1
        while bit < size:
            total = total + swap(total, axis, bit)
            bit *= 2
    for k in range(0, n_col, 2):
        old[k + 1] = [swap(q, "col", 1) for q in old[k]]
    for k in range(0, n_row, inner):
        for j in range(1, inner):
            new[k + j] = swap(new[k], "row", j)

    slots = (tuple(sorted(new)), tuple(sorted(old)))
    place = jnp.stack([lax.axis_index("row"), lax.axis_index("col")]).astype(jnp.int32)
    operands = [new[k] for k in slots[0]] + [q for k in slots[1] for q in old[k]]
    return pl.pallas_call(
        functools.partial(update_kernel, slots, pieces, min(256, piece_rows), float(old_rows * n_row * n_col)),
        in_specs=[smem, smem, smem, vmem] + [vmem] * len(operands) + [hbm],
        out_specs=hbm,
        out_shape=jax.ShapeDtypeStruct(grm.shape, grm.dtype),
        scratch_shapes=[
            pltpu.VMEM(grm.shape, grm.dtype),
            pltpu.VMEM(grm.shape, grm.dtype),
            pltpu.VMEM((grm.shape[1], snps), jnp.bfloat16),
            pltpu.SemaphoreType.DMA((len(slots[1]) * pieces,)),
            pltpu.SemaphoreType.DMA((len(slots[1]) * pieces,)),
        ],
        compiler_params=pltpu.CompilerParams(vmem_limit_bytes=48 * 1024 * 1024),
        name="update",
    )(place, counts, affected, total, *operands, grm)


def solution(mesh):
    in_specs = (
        P(("col", "row"), None),
        P(("row", "col"), None),
        P("row", "col"),
        P("col"),
        P("row", "col"),
    )
    return jax.shard_map(
        on_device, mesh=mesh, in_specs=in_specs, out_specs=P("row", "col"), check_vma=False
    )
```
